32 devices in a mesh: grp: 4 (over y, x), smp: 8 (over z, core).
Axes of the slice: x: 2, y: 2, z: 4, core: 2. Of those that a mesh axis runs over, the one named last changes fastest.
Arguments:
- spins_packed: int32 [32, 8192], P(None, 'smp'), may hold values from -2147483648 to 2147483646
- weight: bfloat16 [1024, 8192], P(None, 'grp'), may hold values from -0.1875 to 0.1875
- hidden_bias: float32 [8192], P('grp'), may hold values from -1.5 to 1.5
- force_w: float32 [1024, 8192], P('smp', 'grp'), may hold values from -6 to 6
- force_b: float32 [8192], P('grp'), may hold values from -6 to 6
Outputs:
- update_w: float32 [1024, 8192], P('smp', 'grp')
- update_b: float32 [8192], P('grp')
The draws below stay inside these ranges and needn't reach their ends.
All inputs are finite; a program needn't handle non-finite values.
Results may differ from the reference program's by a relative error of at most 0.0003.
Values sent between devices are 32-bit elements; how exact they have to be, the bound alone decides.
A program may use at most 64 MiB of HBM per device.

```python
import jax
import jax.numpy as jnp
from jax import lax

NV = 1024
NH = 8192
TOK_DEV = 1024
ITERS = 2
WORDS = 32
TOKENS = 8192


def with_ends(entries, stream_key, low, high):
    dims = entries.shape
    spot = [jax.random.randint(jax.random.fold_in(stream_key, axis), (), 0, dims[axis]) for axis in range(len(dims))]
    entries = entries.at[tuple(spot)].set(low)
    longest = dims.index(max(dims))
    spot[longest] = (spot[longest] + 1) % dims[longest]
    return entries.at[tuple(spot)].set(high)


def block_levels(stream_key, dims, split, smallest, top_value):
    level = 1.0
    for axis_at, shards_of in split:
        heights = jax.random.uniform(jax.random.fold_in(jax.random.fold_in(stream_key, 6), axis_at), (shards_of,), jnp.float32, smallest / len(split), top_value / len(split))
        level = level * jnp.repeat(jnp.exp(heights), dims[axis_at] // shards_of).reshape((-1,) + (1,) * (len(dims) - 1 - axis_at))
    return level


def bell_draw(rng, shape, width, reach, shards=(), kind=jnp.bfloat16):
    array = width * jax.random.normal(rng, shape, jnp.float32)
    if shards:
        array = array * block_levels(rng, shape, shards, -0.22, 0.18)
    return jnp.clip(array, -reach, reach).astype(kind)


def setup_inputs(seed: int = 0) -> dict:
    key_of = jax.random.split(jax.random.key(seed), 6)
    spins_packed = with_ends(jax.random.randint(key_of[0], (WORDS, TOKENS), -2147483648, 2147483647), jax.random.fold_in(key_of[0], 1), -2147483648, 2147483646).astype(jnp.int32)
    weight = bell_draw(key_of[1], (NV, NH), NV ** -0.5, 0.1875, ((1, 4),))
    hidden_bias = jnp.clip(jax.random.uniform(key_of[2], (NH,), jnp.float32, -1.5, 1.5) * block_levels(key_of[2], (NH,), ((0, 4),), -0.4, 0.0), -1.5, 1.5)
    force_w = bell_draw(key_of[3], (NV, NH), 1.0, 6.0, ((0, 8), (1, 4)), jnp.float32)
    force_b = bell_draw(key_of[4], (NH,), 1.0, 6.0, ((0, 4),), jnp.float32)
    return dict(spins_packed=spins_packed, weight=weight, hidden_bias=hidden_bias, force_w=force_w, force_b=force_b)


diag_shift = 0.01


def unpack(packed):
    shifts = jnp.arange(32, dtype=jnp.int32)
    bit_values = jnp.bitwise_and(jnp.right_shift(packed[:, None, :], shifts[None, :, None]), 1)
    signs = 2 * bit_values - 1
    return signs.reshape(packed.shape[0] * 32, packed.shape[1]).astype(jnp.bfloat16)


def reference(spins_packed, weight, hidden_bias, force_w, force_b):
    spins = unpack(spins_packed)
    tile_count = TOKENS // TOK_DEV
    tiles = spins.reshape(NV, tile_count, TOK_DEV).transpose(1, 0, 2)

    def activations(sample_tile):
        pre_activation = jnp.einsum("it,ih->th", sample_tile, weight, preferred_element_type=jnp.float32)
        return jnp.tanh(pre_activation + hidden_bias)

    def forward(direction_w, direction_b):
        def scan_step(running, sample_tile):
            hidden = activations(sample_tile)
            projected = jnp.einsum("it,ih->th", sample_tile, direction_w, precision=lax.Precision.HIGHEST, preferred_element_type=jnp.float32)
            return running, jnp.sum(hidden * (projected + direction_b), axis=1)

        _, sample_values = lax.scan(scan_step, jnp.zeros((), jnp.float32), tiles)
        sample_values = sample_values.reshape(TOKENS)
        return sample_values - jnp.sum(sample_values) / TOKENS

    def metric(centred, direction_w, direction_b):
        scaled = (centred / TOKENS).reshape(tile_count, TOK_DEV)

        def scan_step(running, inputs):
            sample_tile, weights_now = inputs
            hidden = activations(sample_tile)
            weighted = weights_now[:, None] * hidden
            grad_w = running[0] + jnp.einsum("it,th->ih", sample_tile, weighted, precision=lax.Precision.HIGHEST, preferred_element_type=jnp.float32)
            grad_b = running[1] + jnp.dot(weights_now, hidden, precision=lax.Precision.HIGHEST, preferred_element_type=jnp.float32)
            return (grad_w, grad_b), None

        zeros_pair = (jnp.zeros((NV, NH), jnp.float32), jnp.zeros((NH,), jnp.float32))
        (grad_w, grad_b), _ = lax.scan(scan_step, zeros_pair, (tiles, scaled))
        return grad_w + diag_shift * direction_w, grad_b + diag_shift * direction_b

    solution_w = jnp.zeros_like(force_w)
    solution_b = jnp.zeros_like(force_b)
    residual_w, residual_b = force_w, force_b
    direction_w, direction_b = force_w, force_b
    norm_now = jnp.sum(residual_w * residual_w) + jnp.sum(residual_b * residual_b)
    for iteration in range(ITERS):
        centred = forward(direction_w, direction_b)
        curvature = jnp.sum(centred * centred) / TOKENS + diag_shift * (jnp.sum(direction_w * direction_w) + jnp.sum(direction_b * direction_b))
        step_size = norm_now / curvature
        solution_w = solution_w + step_size * direction_w
        solution_b = solution_b + step_size * direction_b
        if iteration + 1 < ITERS:
            image_w, image_b = metric(centred, direction_w, direction_b)
            residual_w = residual_w - step_size * image_w
            residual_b = residual_b - step_size * image_b
            norm_next = jnp.sum(residual_w * residual_w) + jnp.sum(residual_b * residual_b)
            direction_w = residual_w + (norm_next / norm_now) * direction_w
            direction_b = residual_b + (norm_next / norm_now) * direction_b
            norm_now = norm_next
    return solution_w, solution_b
```

```python
import functools

import jax
import jax.numpy as jnp
from jax import lax
from jax.experimental import pallas as pl
from jax.experimental.pallas import tpu as pltpu
from jax.sharding import PartitionSpec as P

MESH = pl.DeviceIdType.MESH
F32, BF16 = jnp.float32, jnp.bfloat16
diag_shift = 0.01
EXTRA = 128
PAD = 16
CHUNKS = 4


def total(x):
    return jnp.sum(jnp.sum(x, axis=0, keepdims=True), axis=1, keepdims=True)


def kernel(
    groups, shards,
    packed_hbm, weight_hbm, bias_ref, force_hbm, force_b_ref,
    out_ref, out_b_ref,
    packed, weight_in, weight_t, bias_t, tile, spins, hidden, force_own, force_pair, lhs, scaled,
    image, image_other, res_own, res_send, res_recv, by_group, by_shard,
    load_sem, spread_send, spread_recv, share_send, share_recv,
    sib_sem, cross_send, cross_recv, relay_send, relay_recv,
    image_send, image_recv, res_send_sem, res_recv_sem,
    group_send, group_recv, shard_send, shard_recv,
):
    grp, smp = lax.axis_index("grp"), lax.axis_index("smp")
    chips = shards // 2
    pairs = chips // 2
    core, chip = lax.rem(smp, 2), smp // 2
    pair_at, side = chip // 2, lax.rem(chip, 2)
    sibling = smp + 1 - 2 * core
    partner = smp + 2 - 4 * side
    words, here = packed_hbm.shape
    rows, units = force_hbm.shape
    half = units // 2
    both = 2 * rows
    wide = 4 * rows
    samples = chips * here
    count = samples * 2
    block = min(512, here)
    part = image.shape[2]
    parts = half // part
    slice_ = here // groups
    chunk = half // CHUNKS
    tiles = here // block
    turns = chips * tiles

    loads = [
        pltpu.make_async_copy(packed_hbm, packed.at[chip], load_sem.at[0]),
        pltpu.make_async_copy(force_hbm, force_own, load_sem.at[1]),
        pltpu.make_async_copy(
            weight_hbm.at[:, pl.ds(pl.multiple_of(side * half, half), half)], weight_in, load_sem.at[2]
        ),
    ]
    for load in loads:
        load.start()

    barrier = pltpu.get_barrier_semaphore()
    for step in range(1, groups):
        pl.semaphore_signal(barrier, device_id={"grp": lax.rem(grp + step, groups)}, device_id_type=MESH)
    for step in range(1, shards):
        pl.semaphore_signal(barrier, device_id={"smp": lax.rem(smp + step, shards)}, device_id_type=MESH)

    def chip_of(step):
        return lax.rem(pair_at + step // 2, pairs) * 2 + lax.rem(side + lax.rem(step, 2), 2)

    def quarter(of):
        return pl.ds(pl.multiple_of(of * slice_, slice_), slice_)

    def spread(step, source, target):
        return pltpu.make_async_remote_copy(
            packed.at[source, :, quarter(grp)], packed.at[source, :, quarter(grp)],
            spread_send.at[step], spread_recv.at[source],
            device_id={"smp": 2 * target + core}, device_id_type=MESH,
        )

    def share(source, step):
        return pltpu.make_async_remote_copy(
            packed.at[source, :, quarter(grp)], packed.at[source, :, quarter(grp)],
            share_send.at[source, step], share_recv.at[source, grp],
            device_id={"grp": lax.rem(grp + step, groups)}, device_id_type=MESH,
        )

    def shared(source, of):
        return pltpu.make_async_remote_copy(
            packed.at[source, :, quarter(of)], packed.at[source, :, quarter(of)],
            share_send.at[source, 0], share_recv.at[source, of],
            device_id={"grp": of}, device_id_type=MESH,
        )

    mine_at = pl.multiple_of(side * half, half)
    theirs_at = pl.multiple_of((1 - side) * half, half)
    mine_cols, their_cols = pl.ds(mine_at, half), pl.ds(theirs_at, half)

    def core_rows(base, of):
        return pl.ds(pl.multiple_of(base + of * rows, rows), rows)

    def sib_copy():
        return pltpu.make_async_remote_copy(
            force_own.at[:, mine_cols], force_pair.at[core_rows(both, core), :], sib_sem.at[0], sib_sem.at[1],
            device_id={"smp": sibling}, device_id_type=MESH,
        )

    def cross(at):
        return pltpu.make_async_remote_copy(
            force_own.at[:, pl.ds(pl.multiple_of(theirs_at + at * chunk, chunk), chunk)],
            force_pair.at[core_rows(0, core), pl.ds(at * chunk, chunk)],
            cross_send.at[at], cross_recv.at[at],
            device_id={"smp": partner}, device_id_type=MESH,
        )

    def relay(at):
        where = force_pair.at[core_rows(0, core), pl.ds(at * chunk, chunk)]
        return pltpu.make_async_remote_copy(
            where, where, relay_send.at[at], relay_recv.at[at],
            device_id={"smp": sibling}, device_id_type=MESH,
        )

    loads[2].wait()
    step_w = min(256, half)

    def turn(at, carry):
        cols = pl.ds(pl.multiple_of(at * step_w, step_w), step_w)
        far = pl.ds(pl.multiple_of(mine_at + at * step_w, step_w), step_w)
        weight_t[cols, :] = weight_in[:, cols].T
        bias_t[cols, :] = jnp.broadcast_to(bias_ref[:, far], (128, step_w)).T
        return carry

    lax.fori_loop(0, half // step_w, turn, 0)
    loads[0].wait()
    loads[1].wait()
    pl.semaphore_wait(barrier, groups + shards - 2)
    for step in range(1, chips):
        spread(step, chip, chip_of(step)).start()
    sib_copy().start()
    for at in range(CHUNKS):
        cross(at).start()

    zero_rows = jnp.zeros((PAD - 1, half), F32)
    lhs[pl.ds(wide, PAD), :] = jnp.concatenate([force_b_ref[:, mine_cols] / pairs, zero_rows], axis=0).astype(BF16)
    mine_force = force_own[:, mine_cols]
    force_pair[core_rows(both, core), :] = mine_force
    lhs[core_rows(both, core), :] = mine_force.astype(BF16)
    sib_copy().wait()
    lhs[core_rows(both, 1 - core), :] = force_pair[core_rows(both, 1 - core), :].astype(BF16)

    shifts = lax.broadcasted_iota(jnp.int32, (32, block), 0)

    def own_values(cols):
        projected = jnp.dot(lhs[both:, :], hidden[:, cols], preferred_element_type=F32)
        value = jnp.sum(projected[:both] * spins[both:, cols].astype(F32), axis=0, keepdims=True)
        return value + projected[both : both + 1]

    def far_values(cols):
        projected = jnp.dot(lhs[:both, :], hidden[:, cols], preferred_element_type=F32)
        return jnp.sum(projected * spins[:both, cols].astype(F32), axis=0, keepdims=True)

    def values_of(cols):
        projected = jnp.dot(lhs[...], hidden[:, cols], preferred_element_type=F32)
        value = jnp.sum(projected[:wide] * spins[:, cols].astype(F32), axis=0, keepdims=True)
        return value + projected[wide : wide + 1]

    unit_block = min(512, half)

    def hidden_block(turn_at, carry):
        step = turn_at // tiles
        at_chip = chip_of(step)
        in_chip = lax.rem(turn_at, tiles)

        def forward(step):
            spread(step, chip_of(step), chip).wait_recv()
            for peer in range(1, groups):
                share(chip_of(step), peer).start()

        @pl.when(turn_at == 1)
        def _():
            forward(1)

        @pl.when(turn_at == min(2, turns - 1))
        def _():
            for step in range(2, chips):
                forward(step)

        @pl.when((in_chip == 0) & (step > 0))
        def _():
            for peer in range(1, groups):
                shared(at_chip, lax.rem(grp + groups - peer, groups)).wait_recv()

        for at in range(CHUNKS):

            @pl.when(turn_at == turns - CHUNKS + at)
            def _(at=at):
                cross(at).wait_recv()
                relay(at).start()

        local = pl.ds(pl.multiple_of(in_chip * block, block), block)
        cols = pl.ds(pl.multiple_of(at_chip * here + in_chip * block, block), block)
        for word in range(words):
            bits = jnp.right_shift(jnp.broadcast_to(packed[at_chip, word : word + 1, local], (32, block)), shifts)
            tile[word * 32 : word * 32 + 32, :] = (2 * jnp.bitwise_and(bits, 1) - 1).astype(F32).astype(BF16)
        spins[:both, cols] = tile[pl.ds(pl.multiple_of((chip + 1 - 2 * side) * both, both), both), :]
        spins[both:, cols] = tile[pl.ds(pl.multiple_of(chip * both, both), both), :]
        for unit in range(0, half, unit_block):
            these = pl.ds(unit, unit_block)
            pre = jnp.dot(weight_t[these, :], tile[...], preferred_element_type=F32)
            bias = bias_t[these, :]
            pre = pre + jnp.concatenate([bias] * (block // 128), axis=1)
            hidden[these, cols] = jnp.tanh(pre).astype(BF16)
        by_group[0, grp, :, cols] = own_values(cols)
        return carry

    lax.fori_loop(0, turns, hidden_block, 0)

    for at in range(CHUNKS):
        relay(at).wait_recv()
    lhs[:both, :] = force_pair[:both, :].astype(BF16)

    def rest_of_values(at, carry):
        cols = pl.ds(pl.multiple_of(at * block, block), block)
        by_group[0, grp, :, cols] = by_group[0, grp, :, cols] + far_values(cols)
        return carry

    lax.fori_loop(0, samples // block, rest_of_values, 0)

    for step in range(1, chips):
        spread(step, chip, chip_of(step)).wait_send()
        for peer in range(1, groups):
            share(chip_of(step), peer).wait_send()
    for at in range(CHUNKS):
        cross(at).wait_send()
        relay(at).wait_send()

    def gather(slots, which, axis, size, me, send, recv):
        copies = []
        for step in range(1, size):
            copies.append(
                pltpu.make_async_remote_copy(
                    slots.at[which, me], slots.at[which, me], send.at[which, step], recv.at[which, me],
                    device_id={axis: lax.rem(me + step, size)}, device_id_type=MESH,
                )
            )
            copies[-1].start()
        for step in range(1, size):
            source = lax.rem(me + size - step, size)
            pltpu.make_async_remote_copy(
                slots.at[which, source], slots.at[which, source], send.at[which, step], recv.at[which, source],
                device_id={axis: source}, device_id_type=MESH,
            ).wait_recv()
        for copy in copies:
            copy.wait_send()

    lane = lax.broadcasted_iota(jnp.int32, (1, EXTRA), 1)

    def reduce_values(which, first, second):
        by_group[which, grp, :, samples:] = jnp.where(lane == 0, first, jnp.where(lane == 1, second, 0.0))
        gather(by_group, which, "grp", groups, grp, group_send, group_recv)
        mine = by_group[which, 0]
        for source in range(1, groups):
            mine = mine + by_group[which, source]
        by_shard[which, smp] = mine
        gather(by_shard, which, "smp", shards, smp, shard_send, shard_recv)
        halves = []
        for parity in range(2):
            value = by_shard[which, parity]
            for source in range(parity + 2, shards, 2):
                value = value + by_shard[which, source]
            halves.append(value)
        extra = halves[0][:, samples:] + halves[1][:, samples:]
        first = jnp.sum(jnp.where(lane == 0, extra, 0.0), axis=1, keepdims=True)
        second = jnp.sum(jnp.where(lane == 1, extra, 0.0), axis=1, keepdims=True)
        return halves[0][:, :samples], halves[1][:, :samples], first, second

    def centre(low, high):
        mean = total(low) / count + total(high) / count
        return low - mean, high - mean

    force_dot = total(force_own[...] * force_own[...]) + total(force_b_ref[...] * force_b_ref[...]) / shards
    low0, high0, norm0, _ = reduce_values(0, force_dot, jnp.zeros((1, 1), F32))
    low, high = centre(low0, high0)
    curvature0 = total(low * low) / count + total(high * high) / count + diag_shift * norm0
    step0 = norm0 / curvature0

    mine = jnp.where(core == 0, low, high)
    for at in range(0, samples, block):
        weights = mine[:, at : at + block]
        scaled[:wide, at : at + block] = (spins[:, at : at + block].astype(F32) * weights).astype(BF16)
        scaled[wide:, at : at + block] = jnp.concatenate(
            [weights, jnp.zeros((PAD - 1, block), F32)], axis=0
        ).astype(BF16)

    def image_copy(at):
        return pltpu.make_async_remote_copy(
            image.at[at], image_other.at[at], image_send.at[at], image_recv.at[at],
            device_id={"smp": sibling}, device_id_type=MESH,
        )

    def image_part(at, carry):
        these = pl.ds(pl.multiple_of(at * part, part), part)
        image[at] = lax.dot_general(
            scaled[...], hidden[these, :], (((1,), (1,)), ((), ())), preferred_element_type=F32
        )
        image_copy(at).start()
        return carry

    lax.fori_loop(0, parts, image_part, 0)

    scale = 1.0 / count
    held = shards // 2

    def res_copy(at):
        return pltpu.make_async_remote_copy(
            res_send.at[at], res_recv.at[at], res_send_sem.at[at], res_recv_sem.at[at],
            device_id={"smp": partner}, device_id_type=MESH,
        )

    def residual_part(at, carry):
        first, second = carry
        these = pl.ds(pl.multiple_of(at * part, part), part)
        image_copy(at).wait()

        def next_residual(which, force):
            whole = image[at, which, :] + image_other[at, which, :]
            return force - step0 * (whole * scale + diag_shift * force)

        force_far, force_near = force_pair[core_rows(0, core), these], force_pair[core_rows(both, core), these]
        far, near = next_residual(core_rows(0, core), force_far), next_residual(core_rows(both, core), force_near)
        force_b = force_b_ref[:, pl.ds(pl.multiple_of(mine_at + at * part, part), part)]
        own_b = next_residual(pl.ds(wide, 1), force_b)
        res_send[at, :rows, :] = far
        res_send[at, rows:, :] = jnp.broadcast_to(own_b, (8, part))
        res_copy(at).start()
        res_own[at, :rows, :] = near
        res_own[at, rows:, :] = jnp.broadcast_to(own_b, (8, part))
        lhs[core_rows(0, core), these] = far.astype(BF16)
        lhs[core_rows(both, core), these] = near.astype(BF16)
        for base in (0, both):
            which = core_rows(base, 1 - core)
            lhs[which, these] = next_residual(which, force_pair[which, these]).astype(BF16)
        lhs[pl.ds(wide, PAD), these] = jnp.concatenate([own_b / pairs, jnp.zeros((PAD - 1, part), F32)], axis=0).astype(BF16)
        first = first + total(far * far) + total(near * near) + total(own_b * own_b) / held
        second = second + total(far * force_far) + total(near * force_near) + total(own_b * force_b) / held
        return first, second

    zero = jnp.zeros((1, 1), F32)
    own_norm, own_cross = lax.fori_loop(0, parts, residual_part, (zero, zero))

    def second_values(at, carry):
        cols = pl.ds(pl.multiple_of(at * block, block), block)
        by_group[1, grp, :, cols] = values_of(cols)
        return carry

    lax.fori_loop(0, samples // block, second_values, 0)
    low1, high1, norm1, crossed = reduce_values(1, own_norm, own_cross)
    beta = norm1 / norm0
    low, high = centre(low1 + beta * low0, high1 + beta * high0)
    direction_dot = norm1 + 2.0 * beta * crossed + beta * beta * norm0
    curvature1 = total(low * low) / count + total(high * high) / count + diag_shift * direction_dot
    step1 = norm1 / curvature1

    of_force = step0 + step1 * beta
    for at in range(parts):
        res_copy(at).wait()
        for base, held_in in ((mine_at, res_own), (theirs_at, res_recv)):
            cols = pl.ds(pl.multiple_of(base + at * part, part), part)
            out_ref[:, cols] = of_force * force_own[:, cols] + step1 * held_in[at, :rows, :]
            out_b_ref[:, cols] = of_force * force_b_ref[:, cols] + step1 * held_in[at, rows : rows + 1, :]


def body(groups, shards, spins_packed, weight, hidden_bias, force_w, force_b):
    words, here = spins_packed.shape
    inputs, units = weight.shape
    rows = force_w.shape[0]
    chips = shards // 2
    samples, wide, half = chips * here, 4 * rows, units // 2
    part = min(256, half)
    parts = half // part
    vmem = pl.BlockSpec(memory_space=pltpu.VMEM)
    hbm = pl.BlockSpec(memory_space=pl.ANY)
    dma = pltpu.SemaphoreType.DMA
    update_w, update_b = pl.pallas_call(
        functools.partial(kernel, groups, shards),
        out_shape=(jax.ShapeDtypeStruct((rows, units), F32), jax.ShapeDtypeStruct((1, units), F32)),
        in_specs=[hbm, hbm, vmem, hbm, vmem],
        out_specs=(vmem, vmem),
        scratch_shapes=[
            pltpu.VMEM((chips, words, here), jnp.int32),
            pltpu.VMEM((inputs, half), BF16),
            pltpu.VMEM((half, inputs), BF16),
            pltpu.VMEM((half, 128), F32),
            pltpu.VMEM((inputs, min(512, here)), BF16),
            pltpu.VMEM((wide, samples), BF16),
            pltpu.VMEM((half, samples), BF16),
            pltpu.VMEM((rows, units), F32),
            pltpu.VMEM((wide, half), F32),
            pltpu.VMEM((wide + PAD, half), BF16),
            pltpu.VMEM((wide + PAD, samples), BF16),
            pltpu.VMEM((parts, wide + PAD, part), F32),
            pltpu.VMEM((parts, wide + PAD, part), F32),
            pltpu.VMEM((parts, rows + 8, part), F32),
            pltpu.VMEM((parts, rows + 8, part), F32),
            pltpu.VMEM((parts, rows + 8, part), F32),
            pltpu.VMEM((2, groups, 1, samples + EXTRA), F32),
            pltpu.VMEM((2, shards, 1, samples + EXTRA), F32),
            dma((3,)),
            dma((chips,)),
            dma((chips,)),
            dma((chips, groups)),
            dma((chips, groups)),
            dma((2,)),
            dma((CHUNKS,)),
            dma((CHUNKS,)),
            dma((CHUNKS,)),
            dma((CHUNKS,)),
            dma((parts,)),
            dma((parts,)),
            dma((parts,)),
            dma((parts,)),
            dma((2, groups)),
            dma((2, groups)),
            dma((2, shards)),
            dma((2, shards)),
        ],
        compiler_params=pltpu.CompilerParams(
            collective_id=0, has_side_effects=True, vmem_limit_bytes=62 * 1024 * 1024
        ),
    )(spins_packed, weight, hidden_bias.reshape(1, -1), force_w, force_b.reshape(1, -1))
    return update_w, update_b.reshape(-1)


def solution(mesh):
    placed = (P(None, "smp"), P(None, "grp"), P("grp"), P("smp", "grp"), P("grp"))
    return jax.shard_map(
        functools.partial(body, mesh.shape["grp"], mesh.shape["smp"]),
        mesh=mesh, in_specs=placed, out_specs=(P("smp", "grp"), P("grp")), check_vma=False,
    )
```

```python
import functools

import jax
import jax.numpy as jnp
from jax import lax
from jax.experimental import pallas as pl
from jax.experimental.pallas import tpu as pltpu
from jax.sharding import PartitionSpec as P

MESH = pl.DeviceIdType.MESH
F32, BF16 = jnp.float32, jnp.bfloat16
diag_shift = 0.01
LANES = 128
PAD = 16
BLOCK = 512
UNITS = 512
PART = 256
LAG = 2
FEW = 32


def total(x):
    return jnp.sum(jnp.sum(x, axis=0, keepdims=True), axis=1, keepdims=True)


def each(low, high, step):
    if high - low <= FEW:
        for at in range(low, high):
            step(at)
    else:
        lax.fori_loop(low, high, lambda at, carry: (step(at), carry)[1], 0)


def kernel(
    groups, shards, pieces,
    packed_hbm, weight_hbm, bias_ref, force_hbm, force_b_ref,
    res_hbm, res_b_ref, coef_ref,
    packed, weight_in, weight_t, bias_t, tile, spins, hidden, force_own, force_other, lhs, scaled,
    image, image_other, residual, values, extras, squares,
    load_sem, packed_send, packed_recv, force_sem, image_send, image_recv, store_sem,
    value_send, value_recv, extra_send, extra_recv, square_sem, ready,
):
    grp, smp = lax.axis_index("grp"), lax.axis_index("smp")
    chips = shards // 2
    pairs = chips // 2
    core, chip = lax.rem(smp, 2), smp // 2
    pair_at, side = chip // 2, lax.rem(chip, 2)
    sibling = smp + 1 - 2 * core
    words, here = packed_hbm.shape
    rows, units = force_hbm.shape
    pair = 2 * rows
    samples = chips * here
    count = samples * 2
    block = tile.shape[1]
    unit_block = min(UNITS, units)
    part = image.shape[2]
    parts = units // part
    tiles = here // block
    turns = chips * tiles
    piece = samples // pieces
    peers = groups * chips
    everyone = groups * shards

    loads = [
        pltpu.make_async_copy(packed_hbm, packed.at[chip], load_sem.at[0]),
        pltpu.make_async_copy(force_hbm, force_own, load_sem.at[1]),
    ]
    loads[0].start()
    weight_loads = []
    for unit in range(0, units, unit_block):
        these = pl.ds(unit, unit_block)
        weight_loads.append(
            pltpu.make_async_copy(weight_hbm.at[:, these], weight_in.at[:, these], load_sem.at[2 + unit // unit_block])
        )
        weight_loads[-1].start()
    loads[1].start()

    barrier = pltpu.get_barrier_semaphore()
    for step in range(1, groups):
        pl.semaphore_signal(barrier, device_id={"grp": lax.rem(grp + step, groups)}, device_id_type=MESH)
    for step in range(1, shards):
        pl.semaphore_signal(barrier, device_id={"smp": lax.rem(smp + step, shards)}, device_id_type=MESH)

    def chip_of(step):
        return lax.rem(pair_at + step // 2, pairs) * 2 + lax.rem(side + lax.rem(step, 2), 2)

    def packed_copy(source, target, at):
        where = packed.at[source, :, pl.ds(pl.multiple_of(at * block, block), block)]
        return pltpu.make_async_remote_copy(
            where, where, packed_send, packed_recv.at[source, at],
            device_id={"smp": 2 * target + core}, device_id_type=MESH,
        )

    force_copy = pltpu.make_async_remote_copy(
        force_own, force_other, force_sem.at[0], force_sem.at[1],
        device_id={"smp": sibling}, device_id_type=MESH,
    )

    def own_rows(of):
        return pl.ds(pl.multiple_of(of * rows, rows), rows)

    shifts = 31 - lax.broadcasted_iota(jnp.int32, (32, block), 0)

    def unpack(at_chip, in_chip, cols):
        local = pl.ds(pl.multiple_of(in_chip * block, block), block)
        for word in range(words):
            bits = lax.shift_left(jnp.broadcast_to(packed[at_chip, word : word + 1, local], (32, block)), shifts)
            tile[word * 32 : word * 32 + 32, :] = jnp.where(bits < 0, 1.0, -1.0).astype(BF16)
        spins[:, cols] = tile[pl.ds(pl.multiple_of(chip * pair, pair), pair), :]

    def activate(unit, cols):
        these = pl.ds(unit, unit_block)
        pre = jnp.dot(weight_t[these, :], tile[...], preferred_element_type=F32)
        bias = bias_t[these, :]
        pre = pre + jnp.concatenate([bias] * (block // LANES), axis=1)
        hidden[these, cols] = jnp.tanh(pre).astype(BF16)

    def columns(at_chip, in_chip):
        return pl.ds(pl.multiple_of(at_chip * here + in_chip * block, block), block)

    def values_of(cols):
        projected = jnp.dot(lhs[...], hidden[:, cols], preferred_element_type=F32)
        value = jnp.sum(projected[:pair] * spins[:, cols].astype(F32), axis=0, keepdims=True)
        return value + projected[pair : pair + 1]

    slot = grp * chips + chip

    def peer_of(step):
        return lax.rem(grp + step // chips, groups), lax.rem(chip + lax.rem(step, chips), chips)

    def value_copy(which, at, source, target):
        where = values.at[which, source, :, pl.ds(pl.multiple_of(at * piece, piece), piece)]
        return pltpu.make_async_remote_copy(
            where, where, value_send.at[which], value_recv.at[which],
            device_id={"grp": target[0], "smp": 2 * target[1] + core}, device_id_type=MESH,
        )

    def send_piece(which, at):
        each(1, peers, lambda step: value_copy(which, at, slot, peer_of(step)).start())

    def all_values(which):
        where = values.at[which, pl.ds(0, peers - 1)]
        return pltpu.make_async_remote_copy(
            where, where, value_send.at[which], value_recv.at[which],
            device_id={"smp": sibling}, device_id_type=MESH,
        )

    def extra_copy(which, source, target):
        return pltpu.make_async_remote_copy(
            extras.at[which, source], extras.at[which, source],
            extra_send.at[which], extra_recv.at[which],
            device_id={"grp": target[0], "smp": target[1]}, device_id_type=MESH,
        )

    def all_extras(which):
        where = extras.at[which, pl.ds(0, everyone - 1)]
        return pltpu.make_async_remote_copy(
            where, where, extra_send.at[which], extra_recv.at[which],
            device_id={"smp": sibling}, device_id_type=MESH,
        )

    def all_packed():
        where = packed.at[pl.ds(0, chips - 1)]
        return pltpu.make_async_remote_copy(
            where, where, packed_send, packed_recv.at[chip, 0],
            device_id={"smp": sibling}, device_id_type=MESH,
        )

    def anyone(step):
        return lax.rem(grp + step // shards, groups), lax.rem(smp + lax.rem(step, shards), shards)

    width = min(256, unit_block)
    loads[0].wait()
    unpack(chip, 0, columns(chip, 0))
    for unit in range(0, units, unit_block):
        weight_loads[unit // unit_block].wait()
        for start in range(unit, unit + unit_block, width):
            weight_t[start : start + width, :] = weight_in[:, start : start + width].T
            bias_t[start : start + width, :] = jnp.broadcast_to(bias_ref[:, start : start + width], (LANES, width)).T
        activate(unit, columns(chip, 0))
    loads[1].wait()
    pl.semaphore_wait(barrier, groups + shards - 2)
    for step in range(1, chips):
        for at in range(tiles):
            packed_copy(chip, chip_of(step), at).start()
    force_copy.start()
    for step in range(1, shards):
        pl.semaphore_signal(ready, device_id={"smp": lax.rem(smp + step, shards)}, device_id_type=MESH)
    for at in range(1, tiles):
        unpack(chip, at, columns(chip, at))
        for unit in range(0, units, unit_block):
            activate(unit, columns(chip, at))

    zero_rows = jnp.zeros((PAD - 1, units), F32)
    lhs[pl.ds(pair, PAD), :] = jnp.concatenate([force_b_ref[...] / chips, zero_rows], axis=0).astype(BF16)
    lhs[own_rows(core), :] = force_own[...].astype(BF16)
    force_dot = total(force_own[...] * force_own[...]) + total(force_b_ref[...] * force_b_ref[...]) / shards
    force_copy.wait()
    lhs[own_rows(1 - core), :] = force_other[...].astype(BF16)
    for at in range(tiles):
        values[0, slot, :, columns(chip, at)] = values_of(columns(chip, at))
    pl.semaphore_wait(ready, shards - 1)
    if pieces == turns:
        for at in range(tiles):
            send_piece(0, chip * tiles + at)

    def remote_tile(turn_at, carry):
        at_chip, in_chip = chip_of(turn_at // tiles), lax.rem(turn_at, tiles)
        cols = columns(at_chip, in_chip)
        packed_copy(at_chip, chip, in_chip).wait_recv()
        unpack(at_chip, in_chip, cols)
        for unit in range(0, units, unit_block):
            activate(unit, cols)
        values[0, slot, :, cols] = values_of(cols)
        if pieces == turns:
            send_piece(0, at_chip * tiles + in_chip)
        return carry
    lax.fori_loop(tiles, turns, remote_tile, 0)
    lane = lax.broadcasted_iota(jnp.int32, (1, LANES), 1)

    def reduce_values(which, first, second):
        if pieces < turns:
            for at in range(pieces):
                send_piece(which, at)
        mine = total(values[which, slot])
        extras[which, grp * shards + smp] = jnp.where(
            lane == 0, first, jnp.where(lane == 1, second, jnp.where(lane == 2, mine, 0.0))
        )
        each(1, everyone, lambda step: extra_copy(which, grp * shards + smp, anyone(step)).start())
        all_values(which).wait_recv()
        value = values[which, 0]
        for source in range(1, peers):
            value = value + values[which, source]
        all_extras(which).wait_recv()
        extra = jnp.sum(extras[which], axis=0)

        def pick(at):
            return jnp.sum(jnp.where(lane == at, extra, 0.0), axis=1, keepdims=True)

        return value, pick(0), pick(1), pick(2)

    def drain(which):
        all_values(which).wait_send()
        all_extras(which).wait_send()

    def square_copy(which):
        return pltpu.make_async_remote_copy(
            squares.at[which, 0], squares.at[which, 1], square_sem.at[which, 0], square_sem.at[which, 1],
            device_id={"smp": sibling}, device_id_type=MESH,
        )

    def square_start(which, centred):
        squares[which, 0] = jnp.broadcast_to(total(centred * centred), (8, LANES))
        square_copy(which).start()

    def square_total(which):
        square_copy(which).wait()
        return (squares[which, 0, 0:1, 0:1] + squares[which, 1, 0:1, 0:1]) / count

    value0, norm0, _, sum0 = reduce_values(0, force_dot, jnp.zeros((1, 1), F32))
    centred = value0 - sum0 / count
    square_start(0, centred)

    weights = centred.astype(BF16)
    for at in range(0, samples, block):
        scaled[:pair, at : at + block] = spins[:, at : at + block] * weights[:, at : at + block]
    scaled[pair:, :] = jnp.concatenate([centred, jnp.zeros((PAD - 1, samples), F32)], axis=0).astype(BF16)

    def image_copy(at):
        return pltpu.make_async_remote_copy(
            image.at[at], image_other.at[at], image_send, image_recv.at[at],
            device_id={"smp": sibling}, device_id_type=MESH,
        )

    def image_part(at):
        these = pl.ds(pl.multiple_of(at * part, part), part)
        image[at] = lax.dot_general(
            scaled[...], hidden[these, :], (((1,), (1,)), ((), ())), preferred_element_type=F32
        )
        image_copy(at).start()

    scale = 1.0 / count

    def store(at):
        cols = pl.ds(pl.multiple_of(at * part, part), part)
        return pltpu.make_async_copy(residual.at[:, cols], res_hbm.at[:, cols], store_sem)

    def residual_part(at, step0, norms):
        first, second = norms
        these = pl.ds(pl.multiple_of(at * part, part), part)
        image_copy(at).wait_recv()

        def next_residual(which, force):
            whole = image[at, which, :] + image_other[at, which, :]
            return force - step0 * (whole * scale + diag_shift * force)

        force = force_own[:, these]
        own = next_residual(own_rows(core), force)
        residual[:, these] = own
        lhs[own_rows(core), these] = own.astype(BF16)
        lhs[own_rows(1 - core), these] = next_residual(own_rows(1 - core), force_other[:, these]).astype(BF16)
        force_b = force_b_ref[:, these]
        own_b = next_residual(pl.ds(pair, 1), force_b)
        res_b_ref[:, these] = own_b
        lhs[pl.ds(pair, PAD), these] = jnp.concatenate([own_b / chips, jnp.zeros((PAD - 1, part), F32)], axis=0).astype(BF16)
        store(at).start()
        first = first + jnp.sum(own * own, axis=0, keepdims=True) + own_b * own_b / shards
        second = second + jnp.sum(own * force, axis=0, keepdims=True) + own_b * force_b / shards
        return first, second

    ahead = min(LAG + 1, parts)
    each(0, ahead, image_part)
    step0 = norm0 / (square_total(0) + diag_shift * norm0)
    drain(0)
    all_packed().wait_send()

    def next_part(at, norms):
        norms = residual_part(at - ahead, step0, norms)
        image_part(at)
        return norms

    none = jnp.zeros((1, part), F32)
    norms = lax.fori_loop(ahead, parts, next_part, (none, none))
    norms = lax.fori_loop(parts - ahead, parts, lambda at, norms: residual_part(at, step0, norms), norms)

    def second_values(at, carry):
        cols = pl.ds(pl.multiple_of(at * block, block), block)
        values[1, slot, :, cols] = values_of(cols)
        if pieces == turns:
            send_piece(1, at)
        return carry

    lax.fori_loop(0, turns, second_values, 0)
    own_norm, own_cross = total(norms[0]), total(norms[1])
    value1, norm1, crossed, sum1 = reduce_values(1, own_norm, own_cross)
    beta = norm1 / norm0
    square_start(1, value1 + beta * value0 - (sum1 + beta * sum0) / count)
    drain(1)
    pltpu.make_async_copy(residual, res_hbm, store_sem).wait()
    pltpu.make_async_remote_copy(
        image, image_other, image_send, image_recv.at[0], device_id={"smp": sibling}, device_id_type=MESH
    ).wait_send()
    direction_dot = norm1 + 2.0 * beta * crossed + beta * beta * norm0
    step1 = norm1 / (square_total(1) + diag_shift * direction_dot)
    coef_ref[...] = jnp.where(lane == 0, step0 + step1 * beta, step1)


def finish(force_ref, force_b_ref, res_ref, res_b_ref, coef_ref, out_ref, out_b_ref):
    of_force, step1 = coef_ref[0:1, 0:1], coef_ref[0:1, 1:2]
    out_ref[...] = of_force * force_ref[...] + step1 * res_ref[...]
    out_b_ref[...] = of_force * force_b_ref[...] + step1 * res_b_ref[...]


def body(groups, shards, spins_packed, weight, hidden_bias, force_w, force_b):
    words, here = spins_packed.shape
    inputs, units = weight.shape
    rows = force_w.shape[0]
    chips = shards // 2
    samples, pair = chips * here, 2 * rows
    part = min(PART, units)
    parts = units // part
    block = min(BLOCK, here)
    turns = samples // block
    peers = groups * chips
    pieces = turns if peers <= FEW else 1
    vmem = pl.BlockSpec(memory_space=pltpu.VMEM)
    hbm = pl.BlockSpec(memory_space=pl.ANY)
    dma = pltpu.SemaphoreType.DMA
    bias_row, force_row = hidden_bias.reshape(1, -1), force_b.reshape(1, -1)
    wide, thin = jax.ShapeDtypeStruct((rows, units), F32), jax.ShapeDtypeStruct((1, units), F32)
    res, res_b, coef = pl.pallas_call(
        functools.partial(kernel, groups, shards, pieces),
        out_shape=(wide, thin, jax.ShapeDtypeStruct((1, LANES), F32)),
        in_specs=[hbm, hbm, vmem, hbm, vmem],
        out_specs=(hbm, vmem, vmem),
        scratch_shapes=[
            pltpu.VMEM((chips, words, here), jnp.int32),
            pltpu.VMEM((inputs, units), BF16),
            pltpu.VMEM((units, inputs), BF16),
            pltpu.VMEM((units, LANES), F32),
            pltpu.VMEM((inputs, block), BF16),
            pltpu.VMEM((pair, samples), BF16),
            pltpu.VMEM((units, samples), BF16),
            pltpu.VMEM((rows, units), F32),
            pltpu.VMEM((rows, units), F32),
            pltpu.VMEM((pair + PAD, units), BF16),
            pltpu.VMEM((pair + PAD, samples), BF16),
            pltpu.VMEM((parts, pair + PAD, part), F32),
            pltpu.VMEM((parts, pair + PAD, part), F32),
            pltpu.VMEM((rows, units), F32),
            pltpu.VMEM((2, peers, 1, samples), F32),
            pltpu.VMEM((2, groups * shards, 1, LANES), F32),
            pltpu.VMEM((2, 2, 8, LANES), F32),
            dma((2 + units // min(UNITS, units),)),
            dma,
            dma((chips, here // block)),
            dma((2,)),
            dma,
            dma((parts,)),
            dma,
            dma((2,)),
            dma((2,)),
            dma((2,)),
            dma((2,)),
            dma((2, 2)),
            pltpu.SemaphoreType.REGULAR,
        ],
        compiler_params=pltpu.CompilerParams(
            collective_id=0, has_side_effects=True, vmem_limit_bytes=67043328
        ),
    )(spins_packed, weight, bias_row, force_w, force_row)
    update_w, update_b = pl.pallas_call(
        finish,
        out_shape=(wide, thin),
        in_specs=[vmem] * 5,
        out_specs=(vmem, vmem),
    )(force_w, force_row, res, res_b, coef)
    return update_w, update_b.reshape(-1)


def solution(mesh):
    placed = (P(None, "smp"), P(None, "grp"), P("grp"), P("smp", "grp"), P("grp"))
    return jax.shard_map(
        functools.partial(body, mesh.shape["grp"], mesh.shape["smp"]),
        mesh=mesh, in_specs=placed, out_specs=(P("smp", "grp"), P("grp")), check_vma=False,
    )
```

```python
import functools

import jax
import jax.numpy as jnp
from jax import lax
from jax.experimental import pallas as pl
from jax.experimental.pallas import tpu as pltpu
from jax.sharding import PartitionSpec as P

MESH = pl.DeviceIdType.MESH
F32, BF16 = jnp.float32, jnp.bfloat16
diag_shift = 0.01
LANES = 128
PAD = 16
BLOCK = 1024
UNITS = 512
PART = 512
LAG = 1
FEW = 32


def total(x):
    return jnp.sum(jnp.sum(x, axis=0, keepdims=True), axis=1, keepdims=True)


def each(low, high, step):
    if high - low <= FEW:
        for at in range(low, high):
            step(at)
    else:
        lax.fori_loop(low, high, lambda at, carry: (step(at), carry)[1], 0)


def kernel(
    groups, shards, pieces,
    packed_hbm, weight_hbm, bias_ref, force_hbm, force_b_ref,
    res_hbm, res_b_ref, coef_ref,
    packed, weight_in, weight_t, bias_t, tile, spins, hidden, force_own, force_other, lhs, scaled,
    image, image_other, residual, values, extras, squares,
    load_sem, packed_send, packed_recv, force_sem, image_send, image_recv, store_sem,
    value_send, value_recv, extra_send, extra_recv, square_sem, ready,
):
    grp, smp = lax.axis_index("grp"), lax.axis_index("smp")
    chips = shards // 2
    pairs = chips // 2
    core, chip = lax.rem(smp, 2), smp // 2
    pair_at, side = chip // 2, lax.rem(chip, 2)
    sibling = smp + 1 - 2 * core
    words, here = packed_hbm.shape
    rows, units = force_hbm.shape
    pair = 2 * rows
    samples = chips * here
    count = samples * 2
    block = tile.shape[1]
    unit_block = min(UNITS, units)
    part = image.shape[2]
    parts = units // part
    tiles = here // block
    turns = chips * tiles
    piece = samples // pieces
    peers = groups * chips
    everyone = groups * shards

    loads = [
        pltpu.make_async_copy(packed_hbm, packed.at[chip], load_sem.at[0]),
        pltpu.make_async_copy(force_hbm, force_own, load_sem.at[1]),
    ]
    loads[0].start()
    weight_loads = []
    for unit in range(0, units, unit_block):
        these = pl.ds(unit, unit_block)
        weight_loads.append(
            pltpu.make_async_copy(weight_hbm.at[:, these], weight_in.at[:, these], load_sem.at[2 + unit // unit_block])
        )
        weight_loads[-1].start()
    loads[1].start()

    barrier = pltpu.get_barrier_semaphore()
    for step in range(1, groups):
        pl.semaphore_signal(barrier, device_id={"grp": lax.rem(grp + step, groups)}, device_id_type=MESH)
    for step in range(1, shards):
        pl.semaphore_signal(barrier, device_id={"smp": lax.rem(smp + step, shards)}, device_id_type=MESH)

    def chip_of(step):
        return lax.rem(pair_at + step // 2, pairs) * 2 + lax.rem(side + lax.rem(step, 2), 2)

    def packed_copy(source, target, at):
        where = packed.at[source, :, pl.ds(pl.multiple_of(at * block, block), block)]
        return pltpu.make_async_remote_copy(
            where, where, packed_send, packed_recv.at[source, at],
            device_id={"smp": 2 * target + core}, device_id_type=MESH,
        )

    force_copy = pltpu.make_async_remote_copy(
        force_own, force_other, force_sem.at[0], force_sem.at[1],
        device_id={"smp": sibling}, device_id_type=MESH,
    )

    def own_rows(of):
        return pl.ds(pl.multiple_of(of * rows, rows), rows)

    shifts = 31 - lax.broadcasted_iota(jnp.int32, (32, block), 0)

    def unpack(at_chip, in_chip, cols):
        local = pl.ds(pl.multiple_of(in_chip * block, block), block)
        for word in range(words):
            bits = lax.shift_left(jnp.broadcast_to(packed[at_chip, word : word + 1, local], (32, block)), shifts)
            tile[word * 32 : word * 32 + 32, :] = jnp.where(bits < 0, 1.0, -1.0).astype(BF16)
        spins[:, cols] = tile[pl.ds(pl.multiple_of(chip * pair, pair), pair), :]

    def activate(unit, cols):
        these = pl.ds(unit, unit_block)
        pre = jnp.dot(weight_t[these, :], tile[...], preferred_element_type=F32)
        bias = bias_t[these, :]
        pre = pre + jnp.concatenate([bias] * (block // LANES), axis=1)
        hidden[these, cols] = jnp.tanh(pre).astype(BF16)

    def columns(at_chip, in_chip):
        return pl.ds(pl.multiple_of(at_chip * here + in_chip * block, block), block)

    def values_of(cols):
        projected = jnp.dot(lhs[...], hidden[:, cols], preferred_element_type=F32)
        value = jnp.sum(projected[:pair] * spins[:, cols].astype(F32), axis=0, keepdims=True)
        return value + projected[pair : pair + 1]

    slot = grp * chips + chip

    def peer_of(step):
        return lax.rem(grp + step // chips, groups), lax.rem(chip + lax.rem(step, chips), chips)

    def value_copy(which, at, source, target):
        where = values.at[which, source, :, pl.ds(pl.multiple_of(at * piece, piece), piece)]
        return pltpu.make_async_remote_copy(
            where, where, value_send.at[which], value_recv.at[which],
            device_id={"grp": target[0], "smp": 2 * target[1] + core}, device_id_type=MESH,
        )

    def send_piece(which, at):
        each(1, peers, lambda step: value_copy(which, at, slot, peer_of(step)).start())

    def all_values(which):
        where = values.at[which, pl.ds(0, peers - 1)]
        return pltpu.make_async_remote_copy(
            where, where, value_send.at[which], value_recv.at[which],
            device_id={"smp": sibling}, device_id_type=MESH,
        )

    def extra_copy(which, source, target):
        return pltpu.make_async_remote_copy(
            extras.at[which, source], extras.at[which, source],
            extra_send.at[which], extra_recv.at[which],
            device_id={"grp": target[0], "smp": target[1]}, device_id_type=MESH,
        )

    def all_extras(which):
        where = extras.at[which, pl.ds(0, everyone - 1)]
        return pltpu.make_async_remote_copy(
            where, where, extra_send.at[which], extra_recv.at[which],
            device_id={"smp": sibling}, device_id_type=MESH,
        )

    def all_packed():
        where = packed.at[pl.ds(0, chips - 1)]
        return pltpu.make_async_remote_copy(
            where, where, packed_send, packed_recv.at[chip, 0],
            device_id={"smp": sibling}, device_id_type=MESH,
        )

    def anyone(step):
        return lax.rem(grp + step // shards, groups), lax.rem(smp + lax.rem(step, shards), shards)

    def meet():
        pl.semaphore_wait(barrier, groups + shards - 2)
        for step in range(1, chips):
            for at in range(tiles):
                packed_copy(chip, chip_of(step), at).start()
        loads[1].wait()
        force_copy.start()
        for step in range(1, shards):
            pl.semaphore_signal(ready, device_id={"smp": lax.rem(smp + step, shards)}, device_id_type=MESH)

    width = min(256, unit_block)
    ahead_units = (units + 1) // 2 if tiles == 1 else units
    loads[0].wait()
    unpack(chip, 0, columns(chip, 0))
    for unit in range(0, units, unit_block):
        weight_loads[unit // unit_block].wait()
        for start in range(unit, unit + unit_block, width):
            weight_t[start : start + width, :] = weight_in[:, start : start + width].T
            bias_t[start : start + width, :] = jnp.broadcast_to(bias_ref[:, start : start + width], (LANES, width)).T
        activate(unit, columns(chip, 0))
        if unit < ahead_units <= unit + unit_block:
            meet()
    for at in range(1, tiles):
        unpack(chip, at, columns(chip, at))
        for unit in range(0, units, unit_block):
            activate(unit, columns(chip, at))

    zero_rows = jnp.zeros((PAD - 1, units), F32)
    lhs[pl.ds(pair, PAD), :] = jnp.concatenate([force_b_ref[...] / chips, zero_rows], axis=0).astype(BF16)
    lhs[own_rows(core), :] = force_own[...].astype(BF16)
    force_dot = total(force_own[...] * force_own[...]) + total(force_b_ref[...] * force_b_ref[...]) / shards
    force_copy.wait()
    lhs[own_rows(1 - core), :] = force_other[...].astype(BF16)
    for at in range(tiles):
        values[0, slot, :, columns(chip, at)] = values_of(columns(chip, at))
    pl.semaphore_wait(ready, shards - 1)
    if pieces == turns:
        for at in range(tiles):
            send_piece(0, chip * tiles + at)

    def remote_tile(turn_at, carry):
        at_chip, in_chip = chip_of(turn_at // tiles), lax.rem(turn_at, tiles)
        cols = columns(at_chip, in_chip)
        packed_copy(at_chip, chip, in_chip).wait_recv()
        unpack(at_chip, in_chip, cols)
        for unit in range(0, units, unit_block):
            activate(unit, cols)
        values[0, slot, :, cols] = values_of(cols)
        if pieces == turns:
            send_piece(0, at_chip * tiles + in_chip)
        return carry
    lax.fori_loop(tiles, turns, remote_tile, 0)
    lane = lax.broadcasted_iota(jnp.int32, (1, LANES), 1)

    def reduce_values(which, first, second):
        if pieces < turns:
            for at in range(pieces):
                send_piece(which, at)
        mine = total(values[which, slot])
        extras[which, grp * shards + smp] = jnp.where(
            lane == 0, first, jnp.where(lane == 1, second, jnp.where(lane == 2, mine, 0.0))
        )
        each(1, everyone, lambda step: extra_copy(which, grp * shards + smp, anyone(step)).start())
        all_values(which).wait_recv()
        value = values[which, 0]
        for source in range(1, peers):
            value = value + values[which, source]
        all_extras(which).wait_recv()
        extra = jnp.sum(extras[which], axis=0)

        def pick(at):
            return jnp.sum(jnp.where(lane == at, extra, 0.0), axis=1, keepdims=True)

        return value, pick(0), pick(1), pick(2)

    def drain(which):
        all_values(which).wait_send()
        all_extras(which).wait_send()

    def square_copy(which):
        return pltpu.make_async_remote_copy(
            squares.at[which, 0], squares.at[which, 1], square_sem.at[which, 0], square_sem.at[which, 1],
            device_id={"smp": sibling}, device_id_type=MESH,
        )

    def square_start(which, centred):
        squares[which, 0] = jnp.broadcast_to(total(centred * centred), (8, LANES))
        square_copy(which).start()

    def square_total(which):
        square_copy(which).wait()
        return (squares[which, 0, 0:1, 0:1] + squares[which, 1, 0:1, 0:1]) / count

    value0, norm0, _, sum0 = reduce_values(0, force_dot, jnp.zeros((1, 1), F32))
    centred = value0 - sum0 / count
    square_start(0, centred)
    weights = centred.astype(BF16)
    for at in range(0, samples, block):
        scaled[:pair, at : at + block] = spins[:, at : at + block] * weights[:, at : at + block]
    scaled[pair:, :] = jnp.concatenate([centred, jnp.zeros((PAD - 1, samples), F32)], axis=0).astype(BF16)

    def image_copy(at):
        return pltpu.make_async_remote_copy(
            image.at[at], image_other.at[at], image_send, image_recv.at[at],
            device_id={"smp": sibling}, device_id_type=MESH,
        )

    def image_part(at):
        these = pl.ds(at * part, part)
        image[at] = lax.dot_general(
            scaled[...], hidden[these, :], (((1,), (1,)), ((), ())), preferred_element_type=F32
        )
        image_copy(at).start()

    scale = 1.0 / count

    def store(at):
        cols = pl.ds(at * part, part)
        return pltpu.make_async_copy(residual.at[:, cols], res_hbm.at[:, cols], store_sem)

    def residual_part(at, step0, norms):
        first, second = norms
        these = pl.ds(at * part, part)
        image_copy(at).wait_recv()

        def next_residual(which, force):
            whole = image[at, which, :] + image_other[at, which, :]
            return force - step0 * (whole * scale + diag_shift * force)

        force = force_own[:, these]
        own = next_residual(own_rows(core), force)
        residual[:, these] = own
        lhs[own_rows(core), these] = own.astype(BF16)
        lhs[own_rows(1 - core), these] = next_residual(own_rows(1 - core), force_other[:, these]).astype(BF16)
        force_b = force_b_ref[:, these]
        own_b = next_residual(pl.ds(pair, 1), force_b)
        res_b_ref[:, these] = own_b
        lhs[pl.ds(pair, PAD), these] = jnp.concatenate([own_b / chips, jnp.zeros((PAD - 1, part), F32)], axis=0).astype(BF16)
        store(at).start()
        first = first + jnp.sum(own * own, axis=0, keepdims=True) + own_b * own_b / shards
        second = second + jnp.sum(own * force, axis=0, keepdims=True) + own_b * force_b / shards
        return first, second

    ahead = min(LAG + 1, parts)
    each(0, ahead, image_part)
    step0 = norm0 / (square_total(0) + diag_shift * norm0)
    drain(0)
    all_packed().wait_send()

    def next_part(at, norms):
        image_part(at)
        return residual_part(at - ahead, step0, norms)

    norms = jnp.zeros((1, part), F32), jnp.zeros((1, part), F32)
    for at in range(ahead, parts):
        norms = next_part(at, norms)
    for at in range(parts - ahead, parts):
        norms = residual_part(at, step0, norms)
    def second_values(at, carry):
        cols = pl.ds(pl.multiple_of(at * block, block), block)
        values[1, slot, :, cols] = values_of(cols)
        if pieces == turns:
            send_piece(1, at)
        return carry

    lax.fori_loop(0, turns, second_values, 0)
    own_norm, own_cross = total(norms[0]), total(norms[1])
    value1, norm1, crossed, sum1 = reduce_values(1, own_norm, own_cross)
    beta = norm1 / norm0
    square_start(1, value1 + beta * value0 - (sum1 + beta * sum0) / count)
    drain(1)
    pltpu.make_async_copy(residual, res_hbm, store_sem).wait()
    pltpu.make_async_remote_copy(
        image, image_other, image_send, image_recv.at[0], device_id={"smp": sibling}, device_id_type=MESH
    ).wait_send()
    direction_dot = norm1 + 2.0 * beta * crossed + beta * beta * norm0
    step1 = norm1 / (square_total(1) + diag_shift * direction_dot)
    coef_ref[...] = jnp.where(lane == 0, step0 + step1 * beta, step1)


def finish(force_ref, force_b_ref, res_ref, res_b_ref, coef_ref, out_ref, out_b_ref):
    of_force, step1 = coef_ref[0:1, 0:1], coef_ref[0:1, 1:2]
    out_ref[...] = of_force * force_ref[...] + step1 * res_ref[...]
    out_b_ref[...] = of_force * force_b_ref[...] + step1 * res_b_ref[...]


def body(groups, shards, spins_packed, weight, hidden_bias, force_w, force_b):
    words, here = spins_packed.shape
    inputs, units = weight.shape
    rows = force_w.shape[0]
    chips = shards // 2
    samples, pair = chips * here, 2 * rows
    part = min(PART, units)
    parts = units // part
    block = min(BLOCK, here)
    turns = samples // block
    peers = groups * chips
    pieces = turns if peers <= FEW else 1
    vmem = pl.BlockSpec(memory_space=pltpu.VMEM)
    hbm = pl.BlockSpec(memory_space=pl.ANY)
    dma = pltpu.SemaphoreType.DMA
    bias_row, force_row = hidden_bias.reshape(1, -1), force_b.reshape(1, -1)
    wide, thin = jax.ShapeDtypeStruct((rows, units), F32), jax.ShapeDtypeStruct((1, units), F32)
    res, res_b, coef = pl.pallas_call(
        functools.partial(kernel, groups, shards, pieces),
        out_shape=(wide, thin, jax.ShapeDtypeStruct((1, LANES), F32)),
        in_specs=[hbm, hbm, vmem, hbm, vmem],
        out_specs=(hbm, vmem, vmem),
        scratch_shapes=[
            pltpu.VMEM((chips, words, here), jnp.int32),
            pltpu.VMEM((inputs, units), BF16),
            pltpu.VMEM((units, inputs), BF16),
            pltpu.VMEM((units, LANES), F32),
            pltpu.VMEM((inputs, block), BF16),
            pltpu.VMEM((pair, samples), BF16),
            pltpu.VMEM((units, samples), BF16),
            pltpu.VMEM((rows, units), F32),
            pltpu.VMEM((rows, units), F32),
            pltpu.VMEM((pair + PAD, units), BF16),
            pltpu.VMEM((pair + PAD, samples), BF16),
            pltpu.VMEM((parts, pair + PAD, part), F32),
            pltpu.VMEM((parts, pair + PAD, part), F32),
            pltpu.VMEM((rows, units), F32),
            pltpu.VMEM((2, peers, 1, samples), F32),
            pltpu.VMEM((2, groups * shards, 1, LANES), F32),
            pltpu.VMEM((2, 2, 8, LANES), F32),
            dma((2 + units // min(UNITS, units),)),
            dma,
            dma((chips, here // block)),
            dma((2,)),
            dma,
            dma((parts,)),
            dma,
            dma((2,)),
            dma((2,)),
            dma((2,)),
            dma((2,)),
            dma((2, 2)),
            pltpu.SemaphoreType.REGULAR,
        ],
        compiler_params=pltpu.CompilerParams(
            collective_id=0, has_side_effects=True, vmem_limit_bytes=67043328
        ),
    )(spins_packed, weight, bias_row, force_w, force_row)
    update_w, update_b = pl.pallas_call(
        finish,
        out_shape=(wide, thin),
        in_specs=[vmem] * 5,
        out_specs=(vmem, vmem),
    )(force_w, force_row, res, res_b, coef)
    return update_w, update_b.reshape(-1)


def solution(mesh):
    placed = (P(None, "smp"), P(None, "grp"), P("grp"), P("smp", "grp"), P("grp"))
    return jax.shard_map(
        functools.partial(body, mesh.shape["grp"], mesh.shape["smp"]),
        mesh=mesh, in_specs=placed, out_specs=(P("smp", "grp"), P("grp")), check_vma=False,
    )
```

```python
import functools

import jax
import jax.numpy as jnp
from jax import lax
from jax.experimental import pallas as pl
from jax.experimental.pallas import tpu as pltpu
from jax.sharding import PartitionSpec as P

MESH = pl.DeviceIdType.MESH
F32, BF16 = jnp.float32, jnp.bfloat16
diag_shift = 0.01
LANES = 128
PAD = 16
BLOCK = 1024
UNITS = 512
PART = 512
LAG = 1
FEW = 32


def total(x):
    return jnp.sum(jnp.sum(x, axis=0, keepdims=True), axis=1, keepdims=True)


def each(low, high, step):
    if high - low <= FEW:
        for at in range(low, high):
            step(at)
    else:
        lax.fori_loop(low, high, lambda at, carry: (step(at), carry)[1], 0)


def kernel(
    groups, shards, pieces,
    packed_hbm, weight_hbm, bias_ref, force_hbm, force_b_ref,
    res_hbm, res_b_ref, coef_ref,
    packed, weight_in, weight_t, bias_t, tile, spins, hidden, force_own, force_other, lhs, scaled,
    image, image_other, residual, values, extras, squares,
    load_sem, packed_send, packed_recv, spread_send, spread_recv, share_send, share_recv, force_sem, image_send, image_recv, store_sem,
    value_send, value_recv, extra_send, extra_recv, square_sem, ready,
):
    grp, smp = lax.axis_index("grp"), lax.axis_index("smp")
    chips = shards // 2
    pairs = chips // 2
    core, chip = lax.rem(smp, 2), smp // 2
    pair_at, side = chip // 2, lax.rem(chip, 2)
    sibling = smp + 1 - 2 * core
    words, here = packed_hbm.shape
    rows, units = force_hbm.shape
    pair = 2 * rows
    samples = chips * here
    count = samples * 2
    block = tile.shape[1]
    unit_block = min(UNITS, units)
    part = image.shape[2]
    parts = units // part
    tiles = here // block
    turns = chips * tiles
    piece = samples // pieces
    peers = groups * chips
    everyone = groups * shards

    loads = [
        pltpu.make_async_copy(packed_hbm, packed.at[chip], load_sem.at[0]),
        pltpu.make_async_copy(force_hbm, force_own, load_sem.at[1]),
    ]
    loads[0].start()
    weight_loads = []
    for unit in range(0, units, unit_block):
        these = pl.ds(unit, unit_block)
        weight_loads.append(
            pltpu.make_async_copy(weight_hbm.at[:, these], weight_in.at[:, these], load_sem.at[2 + unit // unit_block])
        )
        weight_loads[-1].start()
    loads[1].start()

    barrier = pltpu.get_barrier_semaphore()
    for step in range(1, groups):
        pl.semaphore_signal(barrier, device_id={"grp": lax.rem(grp + step, groups)}, device_id_type=MESH)
    for step in range(1, shards):
        pl.semaphore_signal(barrier, device_id={"smp": lax.rem(smp + step, shards)}, device_id_type=MESH)

    def chip_of(step):
        return lax.rem(pair_at + step // 2, pairs) * 2 + lax.rem(side + lax.rem(step, 2), 2)

    def packed_copy(source, target, at):
        where = packed.at[source, :, pl.ds(pl.multiple_of(at * block, block), block)]
        return pltpu.make_async_remote_copy(
            where, where, packed_send, packed_recv.at[source, at],
            device_id={"smp": 2 * target + core}, device_id_type=MESH,
        )

    slice_ = here // groups

    def quarter_copy(source, send, recv, device):
        where = packed.at[source, :, pl.ds(pl.multiple_of(grp * slice_, slice_), slice_)]
        return pltpu.make_async_remote_copy(
            where, where, send, recv.at[source], device_id=device, device_id_type=MESH
        )

    def spread(source, target):
        return quarter_copy(source, spread_send, spread_recv, {"smp": 2 * target + core})

    def share(source, step):
        return quarter_copy(source, share_send, share_recv, {"grp": lax.rem(grp + step, groups)})

    def all_of(sources, columns_of, send, recv):
        where = packed.at[sources, :, pl.ds(0, columns_of)]
        return pltpu.make_async_remote_copy(
            where, where, send, recv, device_id={"smp": sibling}, device_id_type=MESH
        )

    force_copy = pltpu.make_async_remote_copy(
        force_own, force_other, force_sem.at[0], force_sem.at[1],
        device_id={"smp": sibling}, device_id_type=MESH,
    )

    def own_rows(of):
        return pl.ds(pl.multiple_of(of * rows, rows), rows)

    shifts = 31 - lax.broadcasted_iota(jnp.int32, (32, block), 0)

    def unpack(at_chip, in_chip, cols):
        local = pl.ds(pl.multiple_of(in_chip * block, block), block)
        for word in range(words):
            bits = lax.shift_left(jnp.broadcast_to(packed[at_chip, word : word + 1, local], (32, block)), shifts)
            tile[word * 32 : word * 32 + 32, :] = jnp.where(bits < 0, 1.0, -1.0).astype(BF16)
        spins[:, cols] = tile[pl.ds(pl.multiple_of(chip * pair, pair), pair), :]

    def activate(unit, cols):
        these = pl.ds(unit, unit_block)
        pre = jnp.dot(weight_t[these, :], tile[...], preferred_element_type=F32)
        bias = bias_t[these, :]
        pre = pre + jnp.concatenate([bias] * (block // LANES), axis=1)
        hidden[these, cols] = jnp.tanh(pre).astype(BF16)

    def columns(at_chip, in_chip):
        return pl.ds(pl.multiple_of(at_chip * here + in_chip * block, block), block)

    def values_of(cols):
        projected = jnp.dot(lhs[...], hidden[:, cols], preferred_element_type=F32)
        value = jnp.sum(projected[:pair] * spins[:, cols].astype(F32), axis=0, keepdims=True)
        return value + projected[pair : pair + 1]

    slot = grp * chips + chip

    def peer_of(step):
        return lax.rem(grp + step // chips, groups), lax.rem(chip + lax.rem(step, chips), chips)

    def value_copy(which, at, source, target):
        where = values.at[which, source, :, pl.ds(pl.multiple_of(at * piece, piece), piece)]
        return pltpu.make_async_remote_copy(
            where, where, value_send.at[which], value_recv.at[which],
            device_id={"grp": target[0], "smp": 2 * target[1] + core}, device_id_type=MESH,
        )

    def send_piece(which, at):
        each(1, peers, lambda step: value_copy(which, at, slot, peer_of(step)).start())

    def all_values(which):
        where = values.at[which, pl.ds(0, peers - 1)]
        return pltpu.make_async_remote_copy(
            where, where, value_send.at[which], value_recv.at[which],
            device_id={"smp": sibling}, device_id_type=MESH,
        )

    def extra_copy(which, source, target):
        return pltpu.make_async_remote_copy(
            extras.at[which, source], extras.at[which, source],
            extra_send.at[which], extra_recv.at[which],
            device_id={"grp": target[0], "smp": target[1]}, device_id_type=MESH,
        )

    def all_extras(which):
        where = extras.at[which, pl.ds(0, everyone - 1)]
        return pltpu.make_async_remote_copy(
            where, where, extra_send.at[which], extra_recv.at[which],
            device_id={"smp": sibling}, device_id_type=MESH,
        )

    def anyone(step):
        return lax.rem(grp + step // shards, groups), lax.rem(smp + lax.rem(step, shards), shards)

    def meet():
        pl.semaphore_wait(barrier, groups + shards - 2)
        for step in range(2, chips):
            spread(chip, chip_of(step)).start()
        for at in range(tiles):
            packed_copy(chip, chip_of(1), at).start()
        loads[1].wait()
        force_copy.start()
        for step in range(1, shards):
            pl.semaphore_signal(ready, device_id={"smp": lax.rem(smp + step, shards)}, device_id_type=MESH)

    width = min(256, unit_block)
    ahead_units = (units + 1) // 2 if tiles == 1 else units
    loads[0].wait()
    unpack(chip, 0, columns(chip, 0))
    for unit in range(0, units, unit_block):
        weight_loads[unit // unit_block].wait()
        for start in range(unit, unit + unit_block, width):
            weight_t[start : start + width, :] = weight_in[:, start : start + width].T
            bias_t[start : start + width, :] = jnp.broadcast_to(bias_ref[:, start : start + width], (LANES, width)).T
        activate(unit, columns(chip, 0))
        if unit < ahead_units <= unit + unit_block:
            meet()
    for at in range(1, tiles):
        unpack(chip, at, columns(chip, at))
        for unit in range(0, units, unit_block):
            activate(unit, columns(chip, at))

    zero_rows = jnp.zeros((PAD - 1, units), F32)
    lhs[pl.ds(pair, PAD), :] = jnp.concatenate([force_b_ref[...] / chips, zero_rows], axis=0).astype(BF16)
    lhs[own_rows(core), :] = force_own[...].astype(BF16)
    force_dot = total(force_own[...] * force_own[...]) + total(force_b_ref[...] * force_b_ref[...]) / shards
    force_copy.wait()
    lhs[own_rows(1 - core), :] = force_other[...].astype(BF16)
    for at in range(tiles):
        values[0, slot, :, columns(chip, at)] = values_of(columns(chip, at))
    for step in range(2, chips):
        spread(chip_of(step), chip).wait_recv()
        for peer in range(1, groups):
            share(chip_of(step), peer).start()
    pl.semaphore_wait(ready, shards - 1)
    if pieces == turns:
        for at in range(tiles):
            send_piece(0, chip * tiles + at)

    def remote_tile(turn_at, carry):
        at_chip, in_chip = chip_of(turn_at // tiles), lax.rem(turn_at, tiles)
        cols = columns(at_chip, in_chip)

        @pl.when(turn_at < 2 * tiles)
        def _():
            packed_copy(at_chip, chip, in_chip).wait_recv()

        @pl.when((turn_at >= 2 * tiles) & (in_chip == 0))
        def _():
            all_of(at_chip, (groups - 1) * slice_, share_send, share_recv.at[at_chip]).wait_recv()

        unpack(at_chip, in_chip, cols)
        for unit in range(0, units, unit_block):
            activate(unit, cols)
        values[0, slot, :, cols] = values_of(cols)
        if pieces == turns:
            send_piece(0, at_chip * tiles + in_chip)
        return carry
    lax.fori_loop(tiles, turns, remote_tile, 0)
    lane = lax.broadcasted_iota(jnp.int32, (1, LANES), 1)

    def reduce_values(which, first, second):
        if pieces < turns:
            for at in range(pieces):
                send_piece(which, at)
        mine = total(values[which, slot])
        extras[which, grp * shards + smp] = jnp.where(
            lane == 0, first, jnp.where(lane == 1, second, jnp.where(lane == 2, mine, 0.0))
        )
        each(1, everyone, lambda step: extra_copy(which, grp * shards + smp, anyone(step)).start())
        all_values(which).wait_recv()
        value = values[which, 0]
        for source in range(1, peers):
            value = value + values[which, source]
        all_extras(which).wait_recv()
        extra = jnp.sum(extras[which], axis=0)

        def pick(at):
            return jnp.sum(jnp.where(lane == at, extra, 0.0), axis=1, keepdims=True)

        return value, pick(0), pick(1), pick(2)

    def drain(which):
        all_values(which).wait_send()
        all_extras(which).wait_send()

    def square_copy(which):
        return pltpu.make_async_remote_copy(
            squares.at[which, 0], squares.at[which, 1], square_sem.at[which, 0], square_sem.at[which, 1],
            device_id={"smp": sibling}, device_id_type=MESH,
        )

    def square_start(which, centred):
        squares[which, 0] = jnp.broadcast_to(total(centred * centred), (8, LANES))
        square_copy(which).start()

    def square_total(which):
        square_copy(which).wait()
        return (squares[which, 0, 0:1, 0:1] + squares[which, 1, 0:1, 0:1]) / count

    value0, norm0, _, sum0 = reduce_values(0, force_dot, jnp.zeros((1, 1), F32))
    centred = value0 - sum0 / count
    square_start(0, centred)
    weights = centred.astype(BF16)
    for at in range(0, samples, block):
        scaled[:pair, at : at + block] = spins[:, at : at + block] * weights[:, at : at + block]
    scaled[pair:, :] = jnp.concatenate([centred, jnp.zeros((PAD - 1, samples), F32)], axis=0).astype(BF16)

    def image_copy(at):
        return pltpu.make_async_remote_copy(
            image.at[at], image_other.at[at], image_send, image_recv.at[at],
            device_id={"smp": sibling}, device_id_type=MESH,
        )

    def image_part(at):
        these = pl.ds(at * part, part)
        image[at] = lax.dot_general(
            scaled[...], hidden[these, :], (((1,), (1,)), ((), ())), preferred_element_type=F32
        )
        image_copy(at).start()

    scale = 1.0 / count

    def store(at):
        cols = pl.ds(at * part, part)
        return pltpu.make_async_copy(residual.at[:, cols], res_hbm.at[:, cols], store_sem)

    def residual_part(at, step0, norms):
        first, second = norms
        these = pl.ds(at * part, part)
        image_copy(at).wait_recv()

        def next_residual(which, force):
            whole = image[at, which, :] + image_other[at, which, :]
            return force - step0 * (whole * scale + diag_shift * force)

        force = force_own[:, these]
        own = next_residual(own_rows(core), force)
        residual[:, these] = own
        lhs[own_rows(core), these] = own.astype(BF16)
        lhs[own_rows(1 - core), these] = next_residual(own_rows(1 - core), force_other[:, these]).astype(BF16)
        force_b = force_b_ref[:, these]
        own_b = next_residual(pl.ds(pair, 1), force_b)
        res_b_ref[:, these] = own_b
        lhs[pl.ds(pair, PAD), these] = jnp.concatenate([own_b / chips, jnp.zeros((PAD - 1, part), F32)], axis=0).astype(BF16)
        store(at).start()
        first = first + jnp.sum(own * own, axis=0, keepdims=True) + own_b * own_b / shards
        second = second + jnp.sum(own * force, axis=0, keepdims=True) + own_b * force_b / shards
        return first, second

    ahead = min(LAG + 1, parts)
    each(0, ahead, image_part)
    step0 = norm0 / (square_total(0) + diag_shift * norm0)
    drain(0)
    far = pl.ds(0, chips - 2)
    all_of(chip, here, packed_send, packed_recv.at[chip, 0]).wait_send()
    all_of(far, slice_, spread_send, spread_recv.at[chip]).wait_send()
    all_of(far, (groups - 1) * slice_, share_send, share_recv.at[chip]).wait_send()

    def next_part(at, norms):
        image_part(at)
        return residual_part(at - ahead, step0, norms)

    norms = jnp.zeros((1, part), F32), jnp.zeros((1, part), F32)
    for at in range(ahead, parts):
        norms = next_part(at, norms)
    for at in range(parts - ahead, parts):
        norms = residual_part(at, step0, norms)
    def second_values(at, carry):
        cols = pl.ds(pl.multiple_of(at * block, block), block)
        values[1, slot, :, cols] = values_of(cols)
        if pieces == turns:
            send_piece(1, at)
        return carry

    lax.fori_loop(0, turns, second_values, 0)
    own_norm, own_cross = total(norms[0]), total(norms[1])
    value1, norm1, crossed, sum1 = reduce_values(1, own_norm, own_cross)
    beta = norm1 / norm0
    square_start(1, value1 + beta * value0 - (sum1 + beta * sum0) / count)
    drain(1)
    pltpu.make_async_copy(residual, res_hbm, store_sem).wait()
    pltpu.make_async_remote_copy(
        image, image_other, image_send, image_recv.at[0], device_id={"smp": sibling}, device_id_type=MESH
    ).wait_send()
    direction_dot = norm1 + 2.0 * beta * crossed + beta * beta * norm0
    step1 = norm1 / (square_total(1) + diag_shift * direction_dot)
    coef_ref[...] = jnp.where(lane == 0, step0 + step1 * beta, step1)


def finish(force_ref, force_b_ref, res_ref, res_b_ref, coef_ref, out_ref, out_b_ref):
    of_force, step1 = coef_ref[0:1, 0:1], coef_ref[0:1, 1:2]
    out_ref[...] = of_force * force_ref[...] + step1 * res_ref[...]
    out_b_ref[...] = of_force * force_b_ref[...] + step1 * res_b_ref[...]


def body(groups, shards, spins_packed, weight, hidden_bias, force_w, force_b):
    words, here = spins_packed.shape
    inputs, units = weight.shape
    rows = force_w.shape[0]
    chips = shards // 2
    samples, pair = chips * here, 2 * rows
    part = min(PART, units)
    parts = units // part
    block = min(BLOCK, here)
    turns = samples // block
    peers = groups * chips
    pieces = turns if peers <= FEW else 1
    vmem = pl.BlockSpec(memory_space=pltpu.VMEM)
    hbm = pl.BlockSpec(memory_space=pl.ANY)
    dma = pltpu.SemaphoreType.DMA
    bias_row, force_row = hidden_bias.reshape(1, -1), force_b.reshape(1, -1)
    wide, thin = jax.ShapeDtypeStruct((rows, units), F32), jax.ShapeDtypeStruct((1, units), F32)
    res, res_b, coef = pl.pallas_call(
        functools.partial(kernel, groups, shards, pieces),
        out_shape=(wide, thin, jax.ShapeDtypeStruct((1, LANES), F32)),
        in_specs=[hbm, hbm, vmem, hbm, vmem],
        out_specs=(hbm, vmem, vmem),
        scratch_shapes=[
            pltpu.VMEM((chips, words, here), jnp.int32),
            pltpu.VMEM((inputs, units), BF16),
            pltpu.VMEM((units, inputs), BF16),
            pltpu.VMEM((units, LANES), F32),
            pltpu.VMEM((inputs, block), BF16),
            pltpu.VMEM((pair, samples), BF16),
            pltpu.VMEM((units, samples), BF16),
            pltpu.VMEM((rows, units), F32),
            pltpu.VMEM((rows, units), F32),
            pltpu.VMEM((pair + PAD, units), BF16),
            pltpu.VMEM((pair + PAD, samples), BF16),
            pltpu.VMEM((parts, pair + PAD, part), F32),
            pltpu.VMEM((parts, pair + PAD, part), F32),
            pltpu.VMEM((rows, units), F32),
            pltpu.VMEM((2, peers, 1, samples), F32),
            pltpu.VMEM((2, groups * shards, 1, LANES), F32),
            pltpu.VMEM((2, 2, 8, LANES), F32),
            dma((2 + units // min(UNITS, units),)),
            dma,
            dma((chips, here // block)),
            dma,
            dma((chips,)),
            dma,
            dma((chips,)),
            dma((2,)),
            dma,
            dma((parts,)),
            dma,
            dma((2,)),
            dma((2,)),
            dma((2,)),
            dma((2,)),
            dma((2, 2)),
            pltpu.SemaphoreType.REGULAR,
        ],
        compiler_params=pltpu.CompilerParams(
            collective_id=0, has_side_effects=True, vmem_limit_bytes=67043328
        ),
    )(spins_packed, weight, bias_row, force_w, force_row)
    update_w, update_b = pl.pallas_call(
        finish,
        out_shape=(wide, thin),
        in_specs=[vmem] * 5,
        out_specs=(vmem, vmem),
    )(force_w, force_row, res, res_b, coef)
    return update_w, update_b.reshape(-1)


def solution(mesh):
    placed = (P(None, "smp"), P(None, "grp"), P("grp"), P("smp", "grp"), P("grp"))
    return jax.shard_map(
        functools.partial(body, mesh.shape["grp"], mesh.shape["smp"]),
        mesh=mesh, in_specs=placed, out_specs=(P("smp", "grp"), P("grp")), check_vma=False,
    )
```
